32 devices in a mesh: row: 8 (over y, x, core), col: 4 (over z).
Axes of the slice: x: 2, y: 2, z: 4, core: 2. Of those that a mesh axis runs over, the one named last changes fastest.
Arguments:
- state: float32 [9, 35, 8192], P(None, None, ('col', 'row')), may hold values from -6 to 6
- geometry: bfloat16 [9, 128, 8192], P(None, 'row', 'col'), may hold values from -5 to 5
- material: float32 [4, 8192], P(None, ('col', 'row')), may hold values from 0.5 to 2
- neighbours: int32 [4, 4, 8192], P(None, None, ('col', 'row')), may hold values from 0 to 1023, as said below
- send_faces: int32 [32, 4, 64], P(('col', 'row')), may hold values from 0 to 1023, as said below
- vol_eval: float32 [35, 128], replicated, may hold values from -1 to 1
- vol_grad: bfloat16 [3, 35, 128], replicated, may hold values from -0.3125 to 0.3125
- face_eval: float32 [4, 35, 27], replicated, may hold values from -1 to 1
- face_lift: float32 [4, 35, 27], replicated, may hold values from -0.625 to 0.625
- normals: bfloat16 [3, 27, 4, 8192], P(None, None, None, ('col', 'row')), may hold values from -5 to 5
- areas: float32 [27, 4, 8192], P(None, None, ('col', 'row')), may hold values from 0.5 to 2
Outputs:
- section: float32 [9, 35, 8192], P(None, None, ('col', 'row'))
The draws below stay inside these ranges and needn't reach their ends.
Inputs may be any that keep to these rules, and one draw needn't show every extreme that they name: `neighbours`: field 0 is the kind: 0 the neighbour face lies in the same block, 1 in another block of the same row group, 2 free surface, 3 absorbing. Field 1 is the neighbour block's col index (the own col index for kinds 0, 2, 3). Field 2 is, for kind 0, the neighbour's face number f * 256 + e within the block; for kind 1, a slot below the number of faces that the neighbour's block lists for this block in send_faces; else 0. Field 3 is an orientation of 0 to 2 (0 for kinds 2 and 3). Neighbouring is mutual: the neighbour face names this face back, with orientation (3 - turn) % 3. `send_faces`: A block lists at most 64 faces for one col index, the same number as that block lists back, and nothing for its own col index; entries past the count are 0. In every row group some pair of blocks lists exactly 64 faces to each other.
All inputs are finite; a program needn't handle non-finite values.
Results may differ from the reference program's by a relative error of at most 0.0065.
Values may be sent and summed in bfloat16 or wider, within the bound.
No kernel may reach another device: no remote copies, remote signals or barrier semaphores. Data moves between devices by JAX's collectives and lax.ppermute only.
A program may use at most 64 MiB of HBM per device.

```python
import math
import jax
import jax.numpy as jnp
from jax import lax

NQ = 9
NB = 35
VQ = 128
FQ = 27
E_DEV = 256
SLOTS = 64
ELEMENTS = 8192
N_ROW = 8
N_COL = 4


def build_faces(key):
    face_count = 4 * E_DEV
    column_ids = jnp.arange(N_COL, dtype=jnp.int32)
    upper_half = column_ids[:, None] < column_ids[None, :]
    counts = jax.random.randint(jax.random.fold_in(key, 11), (N_ROW, N_COL, N_COL), SLOTS // 4, SLOTS + 1)
    counts = jnp.where(upper_half[None], counts, jnp.transpose(counts, (0, 2, 1)))
    first_col = jax.random.randint(jax.random.fold_in(key, 12), (N_ROW, 1, 1), 0, N_COL)
    second_col = (first_col + jax.random.randint(jax.random.fold_in(key, 13), (N_ROW, 1, 1), 1, N_COL)) % N_COL
    sender = column_ids[None, :, None]
    getter = column_ids[None, None, :]
    filled = (sender == first_col) & (getter == second_col) | (sender == second_col) & (getter == first_col)
    counts = jnp.where(filled, SLOTS, counts)
    counts = jnp.where(sender == getter, 0, counts).astype(jnp.int32)
    pair_turns = jax.random.randint(jax.random.fold_in(key, 14), (N_ROW, N_COL, N_COL, SLOTS), 0, 3)
    pair_turns = jnp.where(upper_half[None, :, :, None], pair_turns, (3 - jnp.transpose(pair_turns, (0, 2, 1, 3))) % 3)

    def one_device(row_id, column_id):
        device_key = jax.random.fold_in(jax.random.fold_in(key, 15), column_id * N_ROW + row_id)
        shuffle = jax.random.permutation(jax.random.fold_in(device_key, 1), face_count).astype(jnp.int32)
        own_counts = counts[row_id, column_id]
        list_ends = jnp.cumsum(own_counts)
        starts = list_ends - own_counts
        remote_total = list_ends[N_COL - 1]
        positions = jnp.arange(face_count, dtype=jnp.int32)
        peer_index = jnp.minimum(jnp.sum((list_ends[None, :] <= positions[:, None]).astype(jnp.int32), axis=1), N_COL - 1)
        slot_index = jnp.clip(positions - starts[peer_index], 0, SLOTS - 1)
        remote = positions < remote_total
        offset = positions - remote_total
        remaining = face_count - remote_total
        edge_total = jax.random.randint(jax.random.fold_in(device_key, 2), (), face_count // 16, face_count // 8 + 1)
        paired = 2 * ((remaining - edge_total) // 2)
        is_pair = (offset >= 0) & (offset < paired)
        partner = jnp.clip(remote_total + jnp.bitwise_xor(jnp.maximum(offset, 0), 1), 0, face_count - 1)
        local_turns = jax.random.randint(jax.random.fold_in(device_key, 3), (face_count,), 0, 3)
        base_turn = local_turns[jnp.clip(remote_total + offset - offset % 2, 0, face_count - 1)]
        pair_turn = jnp.where(offset % 2 == 0, base_turn, (3 - base_turn) % 3)
        edge_kind = 2 + jax.random.randint(jax.random.fold_in(device_key, 4), (face_count,), 0, 2)
        face_kind = jnp.where(remote, 1, jnp.where(is_pair, 0, edge_kind))
        peer_field = jnp.where(remote, peer_index, column_id)
        target = jnp.where(remote, slot_index, jnp.where(is_pair, shuffle[partner], 0))
        turning = jnp.where(remote, pair_turns[row_id, column_id, peer_index, slot_index], jnp.where(is_pair, pair_turn, 0))
        fields = jnp.stack([face_kind, peer_field, target, turning]).astype(jnp.int32)
        by_face = jnp.zeros((4, face_count), jnp.int32).at[:, shuffle].set(fields)
        slot_ids = jnp.arange(SLOTS, dtype=jnp.int32)
        spot_ids = jnp.clip(starts[:, None] + slot_ids[None, :], 0, face_count - 1)
        send_rows = jnp.where(slot_ids[None, :] < own_counts[:, None], shuffle[spot_ids], 0)
        return (by_face.reshape(4, 4, E_DEV), send_rows.astype(jnp.int32))

    def one_column(column_id):

        def per_row(row_id):
            return one_device(row_id, column_id)
        return jax.vmap(per_row)(jnp.arange(N_ROW, dtype=jnp.int32))
    fields, send_rows = jax.vmap(one_column)(column_ids)
    links = jnp.transpose(fields, (2, 3, 0, 1, 4)).reshape(4, 4, N_COL * N_ROW * E_DEV)
    return (links, send_rows.reshape(N_COL * N_ROW, N_COL, SLOTS))


def draw_neighbours(key, part):
    return build_faces(key)[0]


def draw_send_faces(key, part):
    return build_faces(key)[1]


def shard_levels(own_key, shape, pieces, low, high):
    factor_of, own = 1.0, jax.random.fold_in(own_key, 6)
    for position, shards_of in pieces:
        draws = jnp.exp(jax.random.uniform(jax.random.fold_in(own, position), (shards_of,), jnp.float32, low / len(pieces), high / len(pieces)))
        factor_of = factor_of * jnp.repeat(draws, shape[position] // shards_of).reshape([-1 if axis == position else 1 for axis in range(len(shape))])
    return factor_of


def scatter_about(rng, shape, width, limit, split=(), held_as=jnp.bfloat16):
    loudness = shard_levels(rng, shape, split, -0.22, 0.18) if split else 1.0
    values = jax.random.normal(rng, shape, jnp.float32) * width * loudness
    return jnp.minimum(jnp.maximum(values, -limit), limit).astype(held_as)


def setup_inputs(seed: int = 0) -> dict:
    splits = jax.random.split(jax.random.key(seed), 12)
    state = scatter_about(splits[0], (NQ, NB, ELEMENTS), 1.0, 6.0, ((2, 32),), jnp.float32)
    geometry = scatter_about(splits[1], (9, VQ, ELEMENTS), 1.0, 5.0, ((1, 8), (2, 4)))
    material = jnp.clip(jnp.exp(math.log(2.0) - 1.3862944 * jax.random.uniform(splits[2], (4, ELEMENTS), jnp.float32) ** shard_levels(splits[2], (4, ELEMENTS), ((1, 32),), -0.2, 0.2)), 0.5, 2.0)
    neighbours = draw_neighbours(jax.random.fold_in(splits[11], 71), 0)
    send_faces = draw_send_faces(jax.random.fold_in(splits[11], 71), 0)
    vol_eval = scatter_about(splits[5], (NB, VQ), NB ** -0.5, 1.0, (), jnp.float32)
    vol_grad = scatter_about(splits[6], (3, NB, VQ), (3 * VQ) ** -0.5, 0.3125)
    face_eval = scatter_about(splits[7], (4, NB, FQ), NB ** -0.5, 1.0, (), jnp.float32)
    face_lift = scatter_about(splits[8], (4, NB, FQ), (4 * FQ) ** -0.5, 0.625, (), jnp.float32)
    normals = scatter_about(splits[9], (3, FQ, 4, ELEMENTS), 1.0, 5.0, ((3, 32),))
    areas = jnp.clip(jnp.exp(math.log(2.0) - 1.3862944 * jax.random.uniform(splits[10], (FQ, 4, ELEMENTS), jnp.float32) ** shard_levels(splits[10], (FQ, 4, ELEMENTS), ((2, 32),), -0.2, 0.2)), 0.5, 2.0)
    return {"state": state, "geometry": geometry, "material": material, "neighbours": neighbours, "send_faces": send_faces, "vol_eval": vol_eval, "vol_grad": vol_grad, "face_eval": face_eval, "face_lift": face_lift, "normals": normals, "areas": areas}


HIGHEST = lax.Precision.HIGHEST

def normal_flux(values, lame_first, rigidity, buoyancy, normal):
    velocity = values[6:9]
    stress = values[0:6]
    normal_speed = velocity[0] * normal[0] + velocity[1] * normal[1] + velocity[2] * normal[2]
    pressure = lame_first * normal_speed
    components = [-(pressure + 2.0 * rigidity * normal[0] * velocity[0]), -(pressure + 2.0 * rigidity * normal[1] * velocity[1]), -(pressure + 2.0 * rigidity * normal[2] * velocity[2]), -rigidity * (normal[0] * velocity[1] + normal[1] * velocity[0]), -rigidity * (normal[1] * velocity[2] + normal[2] * velocity[1]), -rigidity * (normal[0] * velocity[2] + normal[2] * velocity[0]), -buoyancy * (stress[0] * normal[0] + stress[3] * normal[1] + stress[5] * normal[2]), -buoyancy * (stress[3] * normal[0] + stress[1] * normal[1] + stress[4] * normal[2]), -buoyancy * (stress[5] * normal[0] + stress[4] * normal[1] + stress[2] * normal[2])]
    return jnp.stack(components)

def volume_fluxes(points, metric, material):
    values = points.astype(jnp.float32)
    result = []
    for direction in range(3):
        normal = (metric[3 * direction], metric[3 * direction + 1], metric[3 * direction + 2])
        result.append(normal_flux(values, material[0], material[1], material[2], normal))
    return jnp.stack(result).astype(jnp.bfloat16)

def rotate_points(gathered, turning):
    full_shape = gathered.shape
    grouped = gathered.reshape(full_shape[0], full_shape[1] // 3, 3, full_shape[2], full_shape[3])
    rotated_one = jnp.roll(grouped, -1, axis=2).reshape(full_shape)
    rotated_two = jnp.roll(grouped, -2, axis=2).reshape(full_shape)
    return jnp.where(turning == 0, gathered, jnp.where(turning == 1, rotated_one, rotated_two))

def exterior(traces, gathered, face_kind, turning):
    rotated = rotate_points(gathered, turning)
    mirror = jnp.concatenate([-traces[0:6], traces[6:9]], axis=0)
    return jnp.where(face_kind == 2, mirror, jnp.where(face_kind == 3, 0.0, rotated))

def face_flux(interior, exterior_trace, interior_material, exterior_material, normals, areas):
    normal = (normals[0], normals[1], normals[2])
    interior_flux = normal_flux(interior, interior_material[0], interior_material[1], interior_material[2], normal)
    exterior_flux = normal_flux(exterior_trace, exterior_material[0], exterior_material[1], exterior_material[2], normal)
    interior_speed = jnp.sqrt((interior_material[0] + 2.0 * interior_material[1]) * interior_material[2])
    exterior_speed = jnp.sqrt((exterior_material[0] + 2.0 * exterior_material[1]) * exterior_material[2])
    penalty = 0.5 * jnp.maximum(interior_speed, exterior_speed) * areas
    return 0.5 * (interior_flux + exterior_flux) + penalty * (interior - exterior_trace)

def reference(state, geometry, material, neighbours, send_faces, vol_eval, vol_grad, face_eval, face_lift, normals, areas):
    elem_total = state.shape[2]
    traces = jnp.einsum('fbq,mbe->mqfe', face_eval, state, precision=HIGHEST)
    flat_traces = traces.reshape(9, FQ, 4 * elem_total)
    block_count = N_ROW * N_COL

    def one_block(block_id):
        start = block_id * E_DEV
        column_id = block_id // N_ROW
        row_id = block_id % N_ROW
        own_state = lax.dynamic_slice_in_dim(state, start, E_DEV, 2)
        own_geometry = lax.dynamic_slice_in_dim(geometry, start, E_DEV, 2).astype(jnp.float32)
        own_material = lax.dynamic_slice_in_dim(material, start, E_DEV, 1)
        own_links = lax.dynamic_slice_in_dim(neighbours, start, E_DEV, 2)
        own_traces = lax.dynamic_slice_in_dim(traces, start, E_DEV, 3)
        own_normals = lax.dynamic_slice_in_dim(normals, start, E_DEV, 3).astype(jnp.float32)
        own_areas = lax.dynamic_slice_in_dim(areas, start, E_DEV, 2)
        points = jnp.einsum('bq,mbe->mqe', vol_eval, own_state, precision=HIGHEST).astype(jnp.bfloat16)
        fluxes = volume_fluxes(points, own_geometry, own_material)
        volume = jnp.einsum('dbq,dmqe->mbe', vol_grad.astype(jnp.float32), fluxes.astype(jnp.float32), precision=HIGHEST)
        face_kind = own_links[0]
        peer_index = own_links[1]
        target = own_links[2]
        turning = own_links[3]
        partner_block = (peer_index * N_ROW + row_id).astype(jnp.int32)
        listed = send_faces[partner_block, column_id, jnp.minimum(target, SLOTS - 1)]
        remote_face = listed // E_DEV
        remote_elem = partner_block * E_DEV + listed % E_DEV
        local_face = target // E_DEV
        local_elem = start + target % E_DEV
        own_face = jnp.broadcast_to(jnp.arange(4, dtype=jnp.int32)[:, None], (4, E_DEV))
        own_elem = jnp.broadcast_to(start + jnp.arange(E_DEV, dtype=jnp.int32)[None, :], (4, E_DEV))
        other_face = jnp.where(face_kind == 0, local_face, jnp.where(face_kind == 1, remote_face, own_face))
        other_elem = jnp.where(face_kind == 0, local_elem, jnp.where(face_kind == 1, remote_elem, own_elem))
        global_face = (other_face * elem_total + other_elem).astype(jnp.int32)
        gathered = jnp.take(flat_traces, global_face.reshape(-1), axis=2).reshape(own_traces.shape)
        other_material = jnp.take(material[0:3], other_elem.reshape(-1).astype(jnp.int32), axis=1).reshape(3, 1, 4, E_DEV)
        exterior_trace = exterior(own_traces, gathered, face_kind, turning)
        numeric_flux = face_flux(own_traces, exterior_trace, own_material[0:3][:, None, None, :], other_material, own_normals, own_areas)
        surface = jnp.einsum('fbq,mqfe->mbe', face_lift, numeric_flux, precision=HIGHEST)
        return own_state + own_material[3][None, None, :] * (volume - surface)
    sections = lax.map(one_block, jnp.arange(block_count, dtype=jnp.int32))
    return jnp.transpose(sections, (1, 2, 0, 3)).reshape(9, NB, elem_total)
```

```python
import functools

import jax
import jax.numpy as jnp
from jax import lax
from jax.experimental import pallas as pl
from jax.experimental.pallas import tpu as pltpu
from jax.sharding import PartitionSpec as P


F32 = jnp.float32
BF16 = jnp.bfloat16
I32 = jnp.int32
QP = 32
KB = 48
MAT = 40
GRANT = 12 * 2**20
VMEM = pl.BlockSpec(memory_space=pltpu.VMEM)
ANY = pl.BlockSpec(memory_space=pl.ANY)


def shape_of(shape, dtype):
    return jax.ShapeDtypeStruct(shape, dtype)


def mdot(a, b):
    return jnp.dot(a, b, preferred_element_type=F32)


def swap_groups(x, index, count, width):
    group = lax.broadcasted_iota(I32, x.shape, 1) // width
    step = 1
    while step < count:
        size = x.shape[1]
        up = pltpu.roll(x, size - step * width, 1)
        down = pltpu.roll(x, step * width, 1)
        swapped = jnp.where((group & step) == 0, up, down)
        x = jnp.where((index & step) != 0, swapped, x)
        step *= 2
    return x


def split_kernel(geo, own, mate, sems):
    r = lax.axis_index("row")
    pieces, width = own.shape[0], own.shape[3]
    copies = []
    for j in range(pieces):
        for s, out in enumerate((mate, own)):
            off = pl.multiple_of((r ^ (2 * j + 1 - s)) * width, width)
            copies.append(
                pltpu.make_async_copy(
                    geo.at[:, :, pl.ds(off, width)], out.at[j], sems.at[2 * j + s]
                )
            )
    for c in copies:
        c.start()
    for c in copies:
        c.wait()


def merge_kernel(own, mate, *outs):
    for k, out in enumerate(outs):
        out[0] = own[k]
        out[1] = mate[k]


def pre_kernel(cols, state, material, nbr, send, fe, t0, tp, stack, *rest):
    pieces, (scr, sf, wref) = rest[:-3], rest[-3:]
    c = lax.axis_index("col")
    nb, elems = state.shape[1], state.shape[2]
    fq = fe.shape[2]
    slots = send.shape[2]
    lanes = 4 * QP
    scr[...] = jnp.zeros_like(scr)
    for f in range(4):
        scr[0:nb, QP * f : QP * f + fq] = fe[f]
    base = scr[...]
    lane = lax.broadcasted_iota(I32, base.shape, 1)
    row = lax.broadcasted_iota(I32, base.shape, 0)
    q = lane & (QP - 1)
    k = lax.rem(q, 3)
    unit = ((row >= MAT) & (row < MAT + 3) & (q - fq == row - MAT)).astype(F32)
    inside = q < fq
    one = jnp.where(k < 2, pltpu.roll(base, lanes - 1, 1), pltpu.roll(base, 2, 1))
    two = jnp.where(k == 0, pltpu.roll(base, lanes - 2, 1), pltpu.roll(base, 1, 1))
    blocks = [base + unit, jnp.where(inside, one, 0.0) + unit, jnp.where(inside, two, 0.0) + unit]
    for t, block in enumerate(blocks):
        high = block.astype(BF16).astype(F32)
        wref[lanes * t : lanes * (t + 1), :] = jnp.transpose(
            jnp.concatenate([high, high, block - high], axis=0)
        ).astype(BF16)
    weights = wref[...]
    mat = material[0:3, :]
    mat_high = mat.astype(BF16).astype(F32)
    turn_one, turn_two, stress_sign, speed_sign = [], [], [], []
    for f in range(4):
        kind = nbr[0, f : f + 1, :]
        turn = nbr[3, f : f + 1, :]
        wide = (QP, elems)
        turn_one.append(jnp.broadcast_to(turn, wide) == 2)
        turn_two.append(jnp.broadcast_to(turn, wide) == 1)
        stress_sign.append(
            jnp.broadcast_to(jnp.where(kind == 2, -1.0, jnp.where(kind == 3, 0.0, 1.0)), wide)
        )
        speed_sign.append(jnp.broadcast_to(jnp.where(kind == 3, 0.0, 1.0), wide))
    sf[...] = jnp.zeros_like(sf)
    for m in range(9):
        sf[0:nb, :] = state[m]
        if m == 0:
            sf[MAT : MAT + 3, :] = mat_high
        elif m == 1:
            sf[MAT : MAT + 3, :] = mat - mat_high
        elif m == 2:
            sf[MAT : MAT + 3, :] = jnp.zeros_like(mat)
        full = sf[...]
        high = full.astype(BF16)
        low = (full - high.astype(F32)).astype(BF16)
        block = jnp.concatenate([high, low, high], axis=0)
        stack[m] = block
        traces = mdot(weights, block)
        t0[m] = traces[0:lanes]
        for f in range(4):
            a = traces[QP * f : QP * (f + 1)]
            b = traces[lanes + QP * f : lanes + QP * (f + 1)]
            d = traces[2 * lanes + QP * f : 2 * lanes + QP * (f + 1)]
            chosen = jnp.where(turn_one[f], b, jnp.where(turn_two[f], d, a))
            chosen = chosen * (stress_sign[f] if m < 6 else speed_sign[f])
            tp[f, QP * m : QP * (m + 1), :] = chosen.astype(BF16)
    rows = []
    for d in range(1, cols):
        peer = c + d
        peer = jnp.where(peer >= cols, peer - cols, peer)
        rows.append(send[0, pl.ds(peer, 1), :])
    if len(rows) % 2:
        rows.append(jnp.full((1, slots), -1, I32))
    listed = jnp.concatenate(rows, axis=1)
    total = listed.shape[1]
    elem_ids = lax.broadcasted_iota(I32, (elems, total), 0)
    listed = jnp.broadcast_to(listed, (elems, total))
    out = None
    for f in range(4):
        pick = (elem_ids + f * elems == listed).astype(F32).astype(BF16)
        term = mdot(tp[f], pick)
        out = term if out is None else out + term
    half = out.shape[0] // 2
    left = lax.broadcasted_iota(I32, (half, 2 * slots), 1) < slots
    for d, piece in enumerate(pieces):
        tile = out[:, 2 * slots * (d // 2) : 2 * slots * (d // 2 + 1)]
        top, bottom = tile[:half], tile[half:]
        if d % 2 == 0:
            bottom = pltpu.roll(bottom, slots, 1)
        else:
            top = pltpu.roll(top, slots, 1)
        piece[...] = jnp.where(left, top, bottom).astype(BF16)


def local_kernel(ranks, tp, nbr, stack, material, ve, gl, pv, vscr):
    r = lax.axis_index("row")
    elems = tp.shape[2]
    nb, vq = ve.shape
    elem_ids = lax.broadcasted_iota(I32, (elems, elems), 0)
    own = lax.broadcasted_iota(I32, (1, elems), 1)
    for g in range(4):
        kind = nbr[0, g : g + 1, :]
        target = nbr[2, g : g + 1, :]
        source = jnp.where(kind == 0, target, jnp.where(kind >= 2, own + g * elems, -1))
        source = jnp.broadcast_to(source, (elems, elems))
        total = None
        for f in range(4):
            pick = (elem_ids + f * elems == source).astype(F32).astype(BF16)
            term = mdot(tp[f], pick)
            total = term if total is None else total + term
        gl[g] = total
    vscr[...] = jnp.zeros_like(vscr)
    vscr[0:nb, :] = ve[...]
    vol = swap_groups(vscr[...], r, ranks, vq // ranks)
    high = vol.astype(BF16).astype(F32)
    weights = jnp.transpose(jnp.concatenate([high, high, vol - high], axis=0)).astype(BF16)
    lame = material[0:1, :]
    shear = material[1:2, :]
    buoy = material[2:3, :]
    for m in range(9):
        p = mdot(weights, stack[m]).astype(BF16).astype(F32)
        if m < 6:
            pv[m] = p * -buoy
        else:
            pv[m] = p * -lame
            pv[m + 3] = p * -shear


def place_rows(scr, q, values):
    for t in range(scr.shape[0]):
        scr[t, 4 * q : 4 * q + 4, :] = values[:, 128 * t : 128 * (t + 1)]


def take_rows(scr, f):
    tiles = [scr[t, pl.ds(f, QP, stride=4), :] for t in range(scr.shape[0])]
    return jnp.concatenate(tiles, axis=1)


def surface_kernel(cols, gl, t0, nbr, material, normals, areas, *rest):
    recv, (fs, nscr) = rest[: cols - 1], rest[cols - 1 :]
    c = lax.axis_index("col")
    elems = t0.shape[2]
    fq = areas.shape[0]
    slots = recv[0].shape[1] // 2
    half = recv[0].shape[0]
    left = lax.broadcasted_iota(I32, (half, 2 * slots), 1) < slots
    tiles = []
    for d in range(0, cols - 1, 2):
        a = recv[d][...].astype(F32)
        b = recv[d + 1][...].astype(F32) if d + 1 < cols - 1 else jnp.zeros_like(a)
        top = jnp.where(left, a, pltpu.roll(b, slots, 1))
        bottom = jnp.where(left, pltpu.roll(a, slots, 1), b)
        tiles.append(jnp.concatenate([top, bottom], axis=0).astype(BF16))
    pool = jnp.concatenate(tiles, axis=1)
    pool_ids = lax.broadcasted_iota(I32, (pool.shape[1], elems), 0)
    nscr[...] = jnp.zeros_like(nscr)
    for q in range(fq):
        place_rows(nscr.at[3], q, areas[q])
        for i in range(3):
            place_rows(nscr.at[i], q, normals[i, q].astype(F32))
    own = [material[j : j + 1, :] for j in range(3)]
    own_speed = jnp.sqrt((own[0] + 2.0 * own[1]) * own[2])
    for f in range(4):
        kind = nbr[0, f : f + 1, :]
        hops = c - nbr[1, f : f + 1, :]
        hops = jnp.where(hops < 0, hops + cols, hops)
        source = jnp.where(kind == 1, (hops - 1) * slots + nbr[2, f : f + 1, :], -1)
        pick = (pool_ids == jnp.broadcast_to(source, pool_ids.shape)).astype(F32).astype(BF16)
        outer = gl[f] + mdot(pool, pick)
        other = []
        for j in range(3):
            got = outer[fq + j : fq + j + 1] + outer[QP + fq + j : QP + fq + j + 1]
            other.append(jnp.where(kind >= 2, own[j], got))
        speed = jnp.maximum(own_speed, jnp.sqrt((other[0] + 2.0 * other[1]) * other[2]))
        n = [take_rows(nscr.at[i], f) for i in range(3)]
        penalty = (0.5 * speed) * take_rows(nscr.at[3], f)
        inner = [t0[m, QP * f : QP * (f + 1), :] for m in range(9)]
        outs = [outer[QP * m : QP * (m + 1)] for m in range(9)]
        la, lb = -0.5 * own[0], -0.5 * other[0]
        ga, gb = -0.5 * own[1], -0.5 * other[1]
        wa, wb = -0.5 * own[2], -0.5 * other[2]
        a = [la * inner[6 + i] + lb * outs[6 + i] for i in range(3)]
        v = [ga * inner[6 + i] + gb * outs[6 + i] for i in range(3)]
        s = [wa * inner[i] + wb * outs[i] for i in range(6)]
        flux = fluxes(a, v, s, n)
        for m in range(9):
            value = flux[m] + penalty * (inner[m] - outs[m])
            fs[m, QP * f : QP * (f + 1), :] = value.astype(BF16)


def fluxes(a, v, s, n):
    pressure = n[0] * a[0] + n[1] * a[1] + n[2] * a[2]
    return [
        pressure + 2.0 * (n[0] * v[0]),
        pressure + 2.0 * (n[1] * v[1]),
        pressure + 2.0 * (n[2] * v[2]),
        n[0] * v[1] + n[1] * v[0],
        n[1] * v[2] + n[2] * v[1],
        n[0] * v[2] + n[2] * v[0],
        s[0] * n[0] + s[3] * n[1] + s[5] * n[2],
        s[3] * n[0] + s[1] * n[1] + s[4] * n[2],
        s[5] * n[0] + s[4] * n[1] + s[2] * n[2],
    ]


def final_kernel(ranks, state, material, vg, fl, fs, pv, *rest):
    metric, (out, fx, lscr) = rest[: ranks // 2], rest[ranks // 2 :]
    r = lax.axis_index("row")
    nb, elems = state.shape[1], state.shape[2]
    vq = vg.shape[2]
    fq = fl.shape[2]
    width = vq // ranks
    lscr[...] = jnp.zeros_like(lscr)
    for d in range(3):
        lscr[0:nb, vq * d : vq * (d + 1)] = swap_groups(vg[d].astype(F32), r, ranks, width)
    for f in range(4):
        lscr[0:nb, 3 * vq + QP * f : 3 * vq + QP * f + fq] = -fl[f]
    lift = lscr[...].astype(BF16)
    for p in range(ranks):
        rows = slice(width * p, width * (p + 1))
        s = [pv[i, rows, :] for i in range(6)]
        a = [pv[6 + i, rows, :] for i in range(3)]
        v = [pv[9 + i, rows, :] for i in range(3)]
        for d in range(3):
            n = [metric[p // 2][p % 2, 3 * d + i].astype(F32) for i in range(3)]
            flux = fluxes(a, v, s, n)
            for m in range(9):
                fx[m, vq * d + width * p : vq * d + width * (p + 1), :] = flux[m].astype(BF16)
    step = material[3:4, :]
    for m in range(9):
        change = mdot(lift[:, : 3 * vq], fx[m]) + mdot(lift[:, 3 * vq :], fs[m])
        out[m] = state[m] + step * change[0:nb]


def call(kernel, name, out_shape, in_specs, out_specs, scratch=()):
    return pl.pallas_call(
        kernel,
        out_shape=out_shape,
        in_specs=in_specs,
        out_specs=out_specs,
        scratch_shapes=list(scratch),
        compiler_params=pltpu.CompilerParams(vmem_limit_bytes=GRANT),
        name=name,
    )


def per_device(
    ranks,
    cols,
    state,
    geometry,
    material,
    neighbours,
    send_faces,
    vol_eval,
    vol_grad,
    face_eval,
    face_lift,
    normals,
    areas,
):
    elems = state.shape[2]
    slots = send_faces.shape[2]
    nb, vq = vol_eval.shape
    points = geometry.shape[1]
    chips = ranks // 2
    rows = 9 * QP

    piece = (9, points, elems)
    own, to_mate = call(
        split_kernel,
        "split",
        [shape_of((chips,) + piece, BF16)] * 2,
        [ANY],
        [VMEM] * 2,
        [pltpu.SemaphoreType.DMA((ranks,))],
    )(geometry)
    mate = lax.ppermute(to_mate, "row", [(i, i ^ 1) for i in range(ranks)])

    pre = call(
        functools.partial(pre_kernel, cols),
        "pre",
        [
            shape_of((9, 4 * QP, elems), F32),
            shape_of((4, rows, elems), BF16),
            shape_of((9, 3 * KB, elems), BF16),
        ]
        + [shape_of((rows // 2, 2 * slots), BF16)] * (cols - 1),
        [VMEM] * 5,
        [VMEM] * (cols + 2),
        [
            pltpu.VMEM((KB, 4 * QP), F32),
            pltpu.VMEM((KB, elems), F32),
            pltpu.VMEM((12 * QP, 3 * KB), BF16),
        ],
    )(state, material, neighbours, send_faces, face_eval)
    t0, tp, stack = pre[:3]

    merged = call(
        merge_kernel,
        "merge",
        [shape_of((2,) + piece, BF16)] * chips,
        [VMEM] * 2,
        [VMEM] * chips,
    )(own, mate)
    metric = [merged[0]] + [
        lax.ppermute(merged[k], "row", [(i, i ^ (2 * k)) for i in range(ranks)])
        for k in range(1, chips)
    ]
    received = [
        lax.ppermute(pre[2 + d], "col", [(i, (i + d) % cols) for i in range(cols)])
        for d in range(1, cols)
    ]

    gl, pv = call(
        functools.partial(local_kernel, ranks),
        "local",
        [shape_of((4, rows, elems), F32), shape_of((12, vq, elems), F32)],
        [VMEM] * 5,
        [VMEM] * 2,
        [pltpu.VMEM((KB, vq), F32)],
    )(tp, neighbours, stack, material, vol_eval)

    fs = call(
        functools.partial(surface_kernel, cols),
        "surface",
        shape_of((9, 4 * QP, elems), BF16),
        [VMEM] * (5 + cols),
        VMEM,
        [pltpu.VMEM((4, elems // 128, 4 * QP, 128), F32)],
    )(gl, t0, neighbours, material, normals, areas, *received)

    return call(
        functools.partial(final_kernel, ranks),
        "final",
        shape_of(state.shape, F32),
        [VMEM] * (6 + chips),
        VMEM,
        [
            pltpu.VMEM((9, 3 * vq, elems), BF16),
            pltpu.VMEM((40, 3 * vq + 4 * QP), F32),
        ],
    )(state, material, vol_grad, face_lift, fs, pv, *metric)


def solution(mesh):
    return jax.shard_map(
        functools.partial(per_device, mesh.shape["row"], mesh.shape["col"]),
        mesh=mesh,
        in_specs=(
            P(None, None, ("col", "row")),
            P(None, "row", "col"),
            P(None, ("col", "row")),
            P(None, None, ("col", "row")),
            P(("col", "row"), None, None),
            P(),
            P(),
            P(),
            P(),
            P(None, None, None, ("col", "row")),
            P(None, None, ("col", "row")),
        ),
        out_specs=P(None, None, ("col", "row")),
        check_vma=False,
    )
```
